16 devices in a mesh: dp: 2 (over y, z), fsdp: 8 (over x, core).
Axes of the slice: x: 4, y: 2, z: 1, core: 2. Of those that a mesh axis runs over, the one named last changes fastest.
The devices are a block of a 4x4x8 slice.
Arguments:
- hidden: bfloat16 [16, 64, 2048], P(('dp', 'fsdp')), parts along dimension 0
- attn_norm: bfloat16 [2, 2048], P(None, 'fsdp')
- w_q: bfloat16 [2, 2048, 32, 64], P(None, 'fsdp')
- w_k: bfloat16 [2, 2048, 8, 64], P(None, 'fsdp')
- w_v: bfloat16 [2, 2048, 8, 64], P(None, 'fsdp')
- w_o: bfloat16 [2, 2048, 2048], P(None, 'fsdp')
- mlp_norm: bfloat16 [2, 2048], P(None, 'fsdp')
- w_gate: bfloat16 [2, 2048, 8192], P(None, 'fsdp')
- w_up: bfloat16 [2, 2048, 8192], P(None, 'fsdp')
- w_down: bfloat16 [2, 8192, 2048], P(None, 'fsdp')
Outputs:
- output: bfloat16 [16, 64, 2048], P(('dp', 'fsdp')), parts along dimension 0
There are 2 independent parts. The reference program is written for one: setup_inputs(seed, part) draws one part's arguments, and reference() takes and returns one part's arrays. A program takes and returns all parts, laid end to end along the dimension named above; an argument that names none is the same for every part.
All inputs are finite; a program needn't handle non-finite values.
Results may differ from the reference program's by a relative error of at most 0.02.
Values are sent between devices in bfloat16 or wider.
A program may use at most 768 MiB of HBM per device.

```python
import jax
import jax.numpy as jnp
from jax import lax

MODEL_DIM = 2048
HEADS = 32
KV_HEADS = 8
HEAD_DIM = 64
FFN_DIM = 8192
SEQ_LEN = 64
BATCH_DEV = 1
FSDP_SIZE = 8
LAYERS = 2

GROUP_SEQS = FSDP_SIZE * BATCH_DEV
ROPE_THETA = 500000.0
NORM_EPS = 1e-5


def setup_inputs(seed: int = 0, part: int = 0) -> dict:
    weight_keys = jax.random.split(jax.random.key(seed), 9)
    seq_key = jax.random.fold_in(jax.random.key(seed + 1), part)
    qo_width = HEADS * HEAD_DIM

    def gain_vector(rng_key):
        return (1.0 + 0.25 * jax.random.normal(rng_key, (LAYERS, MODEL_DIM), jnp.float32)).astype(jnp.bfloat16)

    def weight(rng_key, shape, fan_in, gain):
        scale = gain * fan_in ** -0.5
        return (scale * jax.random.normal(rng_key, shape, jnp.float32)).astype(jnp.bfloat16)

    hidden = (0.5 * jax.random.normal(seq_key, (GROUP_SEQS, SEQ_LEN, MODEL_DIM), jnp.float32)).astype(jnp.bfloat16)
    return {
        "hidden": hidden,
        "attn_norm": gain_vector(weight_keys[0]),
        "w_q": weight(weight_keys[1], (LAYERS, MODEL_DIM, HEADS, HEAD_DIM), MODEL_DIM, 1.5),
        "w_k": weight(weight_keys[2], (LAYERS, MODEL_DIM, KV_HEADS, HEAD_DIM), MODEL_DIM, 1.5),
        "w_v": weight(weight_keys[3], (LAYERS, MODEL_DIM, KV_HEADS, HEAD_DIM), MODEL_DIM, 1.0),
        "w_o": weight(weight_keys[4], (LAYERS, qo_width, MODEL_DIM), qo_width, 1.5),
        "mlp_norm": gain_vector(weight_keys[5]),
        "w_gate": weight(weight_keys[6], (LAYERS, MODEL_DIM, FFN_DIM), MODEL_DIM, 1.0),
        "w_up": weight(weight_keys[7], (LAYERS, MODEL_DIM, FFN_DIM), MODEL_DIM, 1.0),
        "w_down": weight(weight_keys[8], (LAYERS, FFN_DIM, MODEL_DIM), FFN_DIM, 1.0),
    }


def rms_norm(hidden, gain):
    wide_hidden = hidden.astype(jnp.float32)
    inv_rms = lax.rsqrt(jnp.mean(wide_hidden * wide_hidden, axis=-1, keepdims=True) + NORM_EPS)
    return (wide_hidden * inv_rms * gain.astype(jnp.float32)).astype(jnp.bfloat16)


def rope_tables(seq_len, head_dim):
    half = head_dim // 2
    inv_freq = jnp.power(ROPE_THETA, -(jnp.arange(half, dtype=jnp.float32) * 2.0 / head_dim))
    angles = jnp.arange(seq_len, dtype=jnp.float32)[:, None] * inv_freq[None, :]
    return jnp.cos(angles)[:, None, :], jnp.sin(angles)[:, None, :]


def apply_rope(proj, cos_table, sin_table):
    half = proj.shape[-1] // 2
    first = proj[..., :half]
    second = proj[..., half:]
    rotated = jnp.concatenate([first * cos_table - second * sin_table, second * cos_table + first * sin_table], axis=-1)
    return rotated.astype(jnp.bfloat16)


def decoder_layer(seq_hidden, weights, cos_table, sin_table):
    attn_gain, w_q, w_k, w_v, w_o, mlp_gain, w_gate, w_up, w_down = weights
    group = HEADS // KV_HEADS
    normed = rms_norm(seq_hidden, attn_gain)
    q_proj = jnp.dot(normed, w_q.reshape(MODEL_DIM, HEADS * HEAD_DIM), preferred_element_type=jnp.float32)
    k_proj = jnp.dot(normed, w_k.reshape(MODEL_DIM, KV_HEADS * HEAD_DIM), preferred_element_type=jnp.float32)
    v_proj = jnp.dot(normed, w_v.reshape(MODEL_DIM, KV_HEADS * HEAD_DIM), preferred_element_type=jnp.float32)
    queries = apply_rope(q_proj.reshape(SEQ_LEN, HEADS, HEAD_DIM), cos_table, sin_table)
    keys_rot = apply_rope(k_proj.reshape(SEQ_LEN, KV_HEADS, HEAD_DIM), cos_table, sin_table)
    values = v_proj.astype(jnp.bfloat16).reshape(SEQ_LEN, KV_HEADS, HEAD_DIM)
    q_grouped = queries.reshape(SEQ_LEN, KV_HEADS, group, HEAD_DIM)
    scores = jnp.einsum("qkgd,skd->kgqs", q_grouped.astype(jnp.float32), keys_rot.astype(jnp.float32)) * HEAD_DIM ** -0.5
    causal = jnp.arange(SEQ_LEN)[:, None] >= jnp.arange(SEQ_LEN)[None, :]
    probs = jax.nn.softmax(jnp.where(causal, scores, -jnp.inf), axis=-1).astype(jnp.bfloat16)
    attended = jnp.einsum("kgqs,skd->qkgd", probs.astype(jnp.float32), values.astype(jnp.float32)).astype(jnp.bfloat16)
    attended = attended.reshape(SEQ_LEN, HEADS * HEAD_DIM)
    after_attn = (seq_hidden.astype(jnp.float32) + jnp.dot(attended, w_o, preferred_element_type=jnp.float32)).astype(jnp.bfloat16)
    mlp_in = rms_norm(after_attn, mlp_gain)
    gate_proj = jnp.dot(mlp_in, w_gate, preferred_element_type=jnp.float32).astype(jnp.bfloat16)
    up_proj = jnp.dot(mlp_in, w_up, preferred_element_type=jnp.float32).astype(jnp.bfloat16)
    gated = (jax.nn.silu(gate_proj.astype(jnp.float32)) * up_proj.astype(jnp.float32)).astype(jnp.bfloat16)
    return (after_attn.astype(jnp.float32) + jnp.dot(gated, w_down, preferred_element_type=jnp.float32)).astype(jnp.bfloat16)


def reference(hidden, attn_norm, w_q, w_k, w_v, w_o, mlp_norm, w_gate, w_up, w_down):
    cos_table, sin_table = rope_tables(SEQ_LEN, HEAD_DIM)
    stacked = (attn_norm, w_q, w_k, w_v, w_o, mlp_norm, w_gate, w_up, w_down)

    def one_sequence(seq_hidden):
        def layer_step(carry, weights):
            return decoder_layer(carry, weights, cos_table, sin_table), None

        final, unused = lax.scan(layer_step, seq_hidden, stacked)
        return final

    return lax.map(one_sequence, hidden)
```

```python
import functools

import jax
import jax.numpy as jnp
import numpy as np
from jax import lax
from jax.experimental import pallas as pl
from jax.experimental.pallas import tpu as pltpu
from jax.sharding import PartitionSpec as P

ROPE_THETA = 500000.0
NORM_EPS = 1e-5
MESH = pl.DeviceIdType.MESH
F32 = jnp.float32
BF16 = jnp.bfloat16

QKV, WO, GATE, UP = range(4)
AX, AO, AM = range(3)
REMOTE = (2, 3, 6, 7, 4, 5)
TAKE = ((256, 128, 128, 128), (128, 128, 128, 128))


def kernel(n, x_hbm, an_ref, mn_ref, tab_hbm, wq, wk, wv, wo, wg, wu, wd, y_ref,
           xf, of, x1f, uf, qkvf, zf, gains, tab, wqkv_v, wo_v, wg_v, wu_v, wd_v, psib, pown, rsib, rrem,
           sw, rw, sf, rf, sa, ra, sg, rg, ss, rs, sr, rr, lsem):
    chips = n // 2
    dp, f = lax.axis_index("dp"), lax.axis_index("fsdp")
    c, k = f // 2, lax.rem(f, 2)
    par = lax.rem(dp, 2)
    partner = dp + 1 - 2 * par
    layers, seq, width = 2, x_hbm.shape[0], x_hbm.shape[1]
    blk = width // n
    tokens = n * seq
    half = tokens // 2
    ffn = wg_v.shape[2]
    heads = 4
    hd = blk // heads

    def chip(d):
        return lax.rem(c + d + chips, chips)

    def to(i):
        return (dp, chip(i // 2) * 2 + lax.rem(k + i % 2, 2))

    def source(i):
        return chip(-(i // 2)) * 2 + lax.rem(k + i % 2, 2)

    def al(v, m):
        return pl.multiple_of(v, m)

    def rc(src, dst, ssem, rsem, dev):
        return pltpu.make_async_remote_copy(src_ref=src, dst_ref=dst, send_sem=ssem, recv_sem=rsem, device_id=dev, device_id_type=MESH)

    def taken(sem, ref):
        pltpu.make_async_copy(ref, ref, sem).wait()

    def block(l, g, src, r0, rows):
        if g == QKV:
            return wqkv_v.at[l, :, pl.ds(al(src * blk + r0, 128), rows)]
        return (None, wo_v, wg_v, wu_v)[g].at[l, pl.ds(al(src * blk + r0, 16), rows), :]

    def pieces(l, g, dst, src, r0, rows):
        if g == QKV:
            cols = pl.ds(al(src * blk + r0, 128), rows)
            mine = pl.ds(al(r0, 128), rows)
            kvd = wk.shape[1] // n
            return [(wq.at[l, pl.ds(al(dst * blk, 16), blk), mine], wqkv_v.at[l, pl.ds(0, blk), cols]),
                    (wk.at[l, pl.ds(al(dst * kvd, 16), kvd), mine], wqkv_v.at[l, pl.ds(blk, kvd), cols]),
                    (wv.at[l, pl.ds(al(dst * kvd, 16), kvd), mine], wqkv_v.at[l, pl.ds(blk + kvd, kvd), cols])]
        w, wide = ((None, None), (wo, blk), (wg, ffn), (wu, ffn))[g]
        return [(w.at[l, pl.ds(al(r0, 16), rows), pl.ds(al(dst * wide, 128), wide)], block(l, g, src, r0, rows))]

    def bytes_of(l, g, rows):
        if g == QKV:
            return wqkv_v.at[l, :, pl.ds(0, rows)]
        return (None, wo_v, wg_v, wu_v)[g].at[l, pl.ds(0, rows), :]

    def issue(l, g, idx):
        for i in idx:
            rows = blk if i == 1 else TAKE[l][g]
            r0 = par * (blk - rows)
            dst = to(i)
            for a, b in pieces(l, g, dst[1], f, r0, rows):
                rc(a, b, sw.at[l, g], rw.at[l, g, i], dst).start()

    def own(l, g):
        for a, b in pieces(l, g, f, f, 0, blk):
            pltpu.make_async_copy(a, b, lsem.at[l, g]).start()

    def arrived(l, g, i):
        rows = blk if i == 1 else TAKE[l][g]
        taken(rw.at[l, g, i], block(l, g, source(i), par * (blk - rows), rows))

    def forward(l, g, idx):
        rows = TAKE[l][g]
        for i in idx:
            arrived(l, g, i)
            if rows < blk:
                there = block(l, g, source(i), par * rows, blk - rows)
                rc(there, there, sf.at[l, g], rf.at[l, g], (partner, f)).start()

    def complete(l, g):
        taken(lsem.at[l, g], bytes_of(l, g, blk))
        arrived(l, g, 1)
        if TAKE[l][g] < blk:
            taken(rf.at[l, g], bytes_of(l, g, len(REMOTE) * (blk - TAKE[l][g])))

    def part(a, src):
        if a == AX:
            return xf.at[pl.ds(al((lax.rem(src, 2) * chips + src // 2) * seq, seq), seq), :]
        return (None, of, x1f)[a].at[:, pl.ds(al(src * blk, 128), blk)]

    def gather_start(l, a, mine=None):
        mine = part(a, f) if mine is None else mine
        for i in (2, 6, 4, 1):
            rc(mine, part(a, f), sa.at[l, a, i], ra.at[l, a, i], to(i)).start()

    def gather_pass(l, a):
        for i in (2, 6, 4):
            got = part(a, source(i))
            taken(ra.at[l, a, i], got)
            rc(got, got, sa.at[l, a, i + 1], ra.at[l, a, i + 1], to(1)).start()

    def gather_end(l, a):
        for i in (1, 3, 7, 5):
            taken(ra.at[l, a, i], part(a, source(i)))
        for i in range(1, n):
            taken(sa.at[l, a, i], part(a, f))

    def norm(src, row):
        step = 32
        gain = gains[pl.ds(row, 1), :]

        @pl.loop(0, tokens // step)
        def _(i):
            at = pl.ds(al(i * step, step), step)
            v = src[at, :].astype(F32)
            inv = lax.rsqrt(jnp.mean(v * v, axis=-1, keepdims=True) + NORM_EPS)
            uf[at, :] = (v * inv * gain).astype(BF16)

    def project(l):
        step = 256

        @pl.loop(0, tokens // step)
        def _(i):
            at = pl.ds(al(i * step, step), step)
            qkvf[at, :] = lax.dot_general(uf[at, :], wqkv_v[l], (((1,), (1,)), ((), ())), preferred_element_type=F32)

    def attend():
        lane = lax.broadcasted_iota(jnp.int32, (seq, 128), 1)
        low = lax.rem(lane, hd) < hd // 2
        first = lane < hd
        head = lax.broadcasted_iota(jnp.int32, (seq, blk), 1) // hd
        qpos = lax.rem(lax.broadcasted_iota(jnp.int32, (heads * seq, seq), 0), seq)
        seen = qpos >= lax.broadcasted_iota(jnp.int32, (heads * seq, seq), 1)

        def rope(v):
            turned = jnp.where(low, pltpu.roll(v, 128 - hd // 2, 1), pltpu.roll(v, hd // 2, 1))
            return v * tab[0] + turned * tab[1]

        @pl.loop(0, n)
        def _(s):
            at = pl.ds(al(s * seq, seq), seq)
            q = jnp.concatenate([rope(qkvf[at, 0:128]), rope(qkvf[at, 128:256])], axis=1)
            kv = qkvf[at, 256:384]
            kr = rope(kv)
            k2 = jnp.where(first, kr, pltpu.roll(kr, hd, 1)).astype(BF16)
            v2 = jnp.where(first, pltpu.roll(kv, hd, 1), kv).astype(BF16)
            k4 = jnp.concatenate([k2, k2], axis=1)
            v4 = jnp.concatenate([v2, v2], axis=1)
            q4 = jnp.concatenate([jnp.where(head == h, q, 0.0) for h in range(heads)], axis=0).astype(BF16)
            score = lax.dot_general(q4, k4, (((1,), (1,)), ((), ())), preferred_element_type=F32) * hd ** -0.5
            score = jnp.where(seen, score, -jnp.inf)
            e = jnp.exp(score - jnp.max(score, axis=-1, keepdims=True))
            prob = (e / jnp.sum(e, axis=-1, keepdims=True)).astype(BF16)
            o4 = jnp.dot(prob, v4, preferred_element_type=F32)
            o = o4[0:seq]
            for h in range(1, heads):
                o = jnp.where(head == h, o4[h * seq:(h + 1) * seq], o)
            of[at, pl.ds(al(f * blk, 128), blk)] = o.astype(BF16)

    def output_projection(l):
        step = 256

        @pl.loop(0, tokens // step)
        def _(i):
            at = pl.ds(al(i * step, step), step)
            cols = pl.ds(al(f * blk, 128), blk)
            acc = jnp.dot(of[at, :], wo_v[l], preferred_element_type=F32)
            x1f[at, cols] = (xf[at, cols].astype(F32) + acc).astype(BF16)

    def gate_up(l):
        step = 256

        @pl.loop(0, ffn // step)
        def _(i):
            at = pl.ds(al(i * step, step), step)
            a = jnp.dot(uf[...], wg_v[l, :, at], preferred_element_type=F32).astype(BF16).astype(F32)
            b = jnp.dot(uf[...], wu_v[l, :, at], preferred_element_type=F32).astype(BF16).astype(F32)
            zf[:, at] = (a * jax.nn.sigmoid(a) * b).astype(BF16)

    dtile = psib.shape[1] // 4

    def down_start(l):
        for t in range(4):
            cols = pl.ds(t * dtile, dtile)
            psib[:, cols] = jnp.dot(zf[pl.ds(al((1 - k) * half, half), half), :], wd_v[l, :, cols], preferred_element_type=F32)
            rc(psib.at[:, cols], rsib.at[:, cols], ss.at[l, t], rs.at[l, t], to(1)).start()
        for t in range(4):
            cols = pl.ds(t * dtile, dtile)
            acc = jnp.dot(zf[pl.ds(al(k * half, half), half), :], wd_v[l, :, cols], preferred_element_type=F32)
            taken(rs.at[l, t], rsib.at[:, cols])
            pown[:, cols] = acc + rsib[:, cols]
            for d in (1, 3, 2):
                rows = pl.ds(al(chip(d) * seq, seq), seq)
                rc(pown.at[rows, cols], rrem.at[d, :, cols], sr.at[l, t, d], rr.at[l, t, d], to(2 * d)).start()

    def down_end(l, out):
        mine = pl.ds(al(c * seq, seq), seq)
        at = pl.ds(al((k * chips + c) * seq, seq), seq)
        for t in range(4):
            cols = pl.ds(t * dtile, dtile)
            for d in (1, 3, 2):
                taken(rr.at[l, t, d], rrem.at[d, :, cols])
            acc = pown[mine, cols] + rrem[1, :, cols] + (rrem[3, :, cols] + rrem[2, :, cols])
            out(cols, (x1f[at, cols].astype(F32) + acc).astype(BF16))

    def down_sent(l):
        for t in range(4):
            cols = pl.ds(t * dtile, dtile)
            taken(ss.at[l, t], psib.at[:, cols])
            for d in (1, 3, 2):
                taken(sr.at[l, t, d], rrem.at[d, :, cols])

    gains[...] = jnp.zeros_like(gains)
    mycols = pl.ds(al(f * blk, 128), blk)
    gains[0:2, mycols] = an_ref[...].astype(F32)
    gains[2:4, mycols] = mn_ref[...].astype(F32)
    gblock = gains.at[:, mycols]
    local_x = pltpu.make_async_copy(x_hbm, part(AX, f), lsem.at[0, 4])
    local_x.start()
    local_tab = pltpu.make_async_copy(tab_hbm, tab, lsem.at[1, 4])
    local_tab.start()
    own(0, QKV)

    barrier = pltpu.get_barrier_semaphore()
    for i in range(1, n):
        pl.semaphore_signal(barrier, inc=1, device_id=to(i), device_id_type=MESH)
    pl.semaphore_signal(barrier, inc=1, device_id=(partner, f), device_id_type=MESH)
    pl.semaphore_wait(barrier, n)

    gather_start(0, AX, x_hbm)
    issue(0, QKV, REMOTE + (1,))
    for i in range(1, n):
        rc(gblock, gblock, sg.at[i], rg.at[i], to(i)).start()
    for g in (WO, GATE, UP):
        own(0, g)
    issue(0, WO, REMOTE + (1,))
    issue(0, GATE, REMOTE[:4] + (1,))
    own_d = [pltpu.make_async_copy(wd.at[l], wd_v.at[l], lsem.at[l, 5]) for l in range(layers)]
    own_d[0].start()

    for l in range(layers):
        if l == 0:
            local_x.wait()
            local_tab.wait()
            for i in range(1, n):
                taken(rg.at[i], gains.at[:, pl.ds(al(source(i) * blk, 128), blk)])
        gather_pass(l, AX)
        gather_end(l, AX)
        norm(xf, l)
        if TAKE[l][QKV] == blk:
            forward(l, QKV, REMOTE)
        complete(l, QKV)
        project(l)
        attend()
        gather_start(l, AO)
        issue(l, GATE, REMOTE[4:])
        issue(l, UP, REMOTE[:4] + (1,))
        forward(l, WO, REMOTE)
        forward(l, GATE, REMOTE[:4])
        gather_pass(l, AO)
        gather_end(l, AO)
        complete(l, WO)
        output_projection(l)
        gather_start(l, AM)
        issue(l, UP, REMOTE[4:])
        forward(l, GATE, REMOTE[4:])
        forward(l, UP, REMOTE[:4])
        gather_pass(l, AM)
        gather_end(l, AM)
        norm(x1f, layers + l)
        forward(l, UP, REMOTE[4:])
        if l + 1 < layers:
            issue(l + 1, QKV, REMOTE + (1,))
            for g in range(4):
                own(l + 1, g)
            own_d[l + 1].start()
        complete(l, GATE)
        complete(l, UP)
        gate_up(l)
        own_d[l].wait()
        down_start(l)
        if l + 1 < layers:
            issue(l + 1, WO, REMOTE + (1,))
            forward(l + 1, QKV, REMOTE)

            def store(cols, v):
                xf[pl.ds(al((k * chips + c) * seq, seq), seq), cols] = v

            down_end(l, store)
            down_sent(l)
            gather_start(l + 1, AX)
            issue(l + 1, GATE, REMOTE[:4] + (1,))
        else:
            def store(cols, v):
                y_ref[:, cols] = v

            down_end(l, store)
            down_sent(l)

    for i in range(1, n):
        taken(sg.at[i], gblock)
    for l in range(layers):
        for g in range(4):
            taken(sw.at[l, g], bytes_of(l, g, len(REMOTE) * TAKE[l][g] + blk))
            if TAKE[l][g] < blk:
                taken(sf.at[l, g], bytes_of(l, g, len(REMOTE) * (blk - TAKE[l][g])))


def rope_tables(seq, hd):
    inv_freq = np.power(np.float32(ROPE_THETA), -(np.arange(hd // 2, dtype=np.float32) * np.float32(2.0) / np.float32(hd)))
    angles = np.arange(seq, dtype=np.float32)[:, None] * inv_freq[None, :].astype(np.float32)
    cos, sin = np.cos(angles), np.sin(angles)
    cos = np.concatenate([cos, cos] * (128 // hd), axis=1)
    sin = np.concatenate([-sin, sin] * (128 // hd), axis=1)
    return np.stack([cos, sin]).astype(np.float32)


def solution(mesh):
    n = mesh.shape["fsdp"]
    batch_spec = P(("dp", "fsdp"), None, None)
    gain_spec = P(None, "fsdp")
    proj_spec = P(None, "fsdp", None, None)
    mat_spec = P(None, "fsdp", None)

    def local_forward(hidden, attn_norm, w_q, w_k, w_v, w_o, mlp_norm, w_gate, w_up, w_down):
        seq, width = hidden.shape[1], hidden.shape[2]
        layers, blk, hd = w_q.shape[0], w_q.shape[1], w_q.shape[3]
        tokens, ffn = n * seq, w_gate.shape[2] // n
        half = tokens // 2
        qkv = (w_q.shape[2] + 2 * w_k.shape[2]) * hd // n

        def turn(w):
            return jnp.transpose(w, (0, 2, 3, 1)).reshape(layers, w.shape[2] * hd, blk)

        tables = jnp.asarray(rope_tables(seq, hd))
        anyspace = pl.BlockSpec(memory_space=pl.ANY)
        vmem = pl.BlockSpec(memory_space=pltpu.VMEM)
        dma = pltpu.SemaphoreType.DMA
        out = pl.pallas_call(
            functools.partial(kernel, n),
            out_shape=jax.ShapeDtypeStruct((seq, width), BF16),
            in_specs=[anyspace, vmem, vmem] + [anyspace] * 8,
            out_specs=vmem,
            scratch_shapes=[
                pltpu.VMEM((tokens, width), BF16),
                pltpu.VMEM((tokens, width), BF16),
                pltpu.VMEM((tokens, width), BF16),
                pltpu.VMEM((tokens, width), BF16),
                pltpu.VMEM((tokens, qkv), F32),
                pltpu.VMEM((tokens, ffn), BF16),
                pltpu.VMEM((8, width), F32),
                pltpu.VMEM((2, seq, 128), F32),
                pltpu.VMEM((layers, qkv, width), BF16),
                pltpu.VMEM((layers, width, blk), BF16),
                pltpu.VMEM((layers, width, ffn), BF16),
                pltpu.VMEM((layers, width, ffn), BF16),
                pltpu.VMEM((layers, ffn, width), BF16),
                pltpu.VMEM((half, width), F32),
                pltpu.VMEM((half, width), F32),
                pltpu.VMEM((half, width), F32),
                pltpu.VMEM((4, seq, width), F32),
                dma((layers, 4)), dma((layers, 4, n)),
                dma((layers, 4)), dma((layers, 4)),
                dma((layers, 3, n)), dma((layers, 3, n)),
                dma((n,)), dma((n,)),
                dma((layers, 4)), dma((layers, 4)),
                dma((layers, 4, 4)), dma((layers, 4, 4)),
                dma((layers, 6)),
            ],
            compiler_params=pltpu.CompilerParams(collective_id=0, has_side_effects=True, vmem_limit_bytes=63 * 2**20),
        )(hidden[0], attn_norm, mlp_norm, tables, turn(w_q), turn(w_k), turn(w_v), w_o, w_gate, w_up, w_down)
        return out[None]

    return jax.shard_map(local_forward, mesh=mesh, in_specs=(batch_spec, gain_spec, proj_spec, proj_spec, proj_spec, mat_spec, gain_spec, mat_spec, mat_spec, mat_spec), out_specs=batch_spec, check_vma=False)
```

```python
import functools

import jax
import jax.numpy as jnp
import numpy as np
from jax import lax
from jax.experimental import pallas as pl
from jax.experimental.pallas import tpu as pltpu
from jax.sharding import PartitionSpec as P

ROPE_THETA = 500000.0
NORM_EPS = 1e-5
MESH = pl.DeviceIdType.MESH
F32 = jnp.float32
BF16 = jnp.bfloat16

QKV, WO, G0, G1, U0, U1 = range(6)
AX, AO, AM = range(3)
REMOTE = (2, 3, 6, 7, 4, 5)
SAME, CROSS, NEAR, FAR = (2, 6), (3, 7), REMOTE[:4], REMOTE[4:] + (1,)
ALL = REMOTE + (1,)
GROUPS = 6
SPLIT = 4
TILES = 8
TAKE = ((128, 128, 128, 128, 128, 128), (128, 128, 128, 128, 128, 128))


def kernel(n, x_hbm, an_ref, mn_ref, tab_hbm, wq, wk, wv, wo, wg, wu, wd, y_ref,
           xf, of, x1f, uf, qkvf, zf, gains, tab, wqkv_v, wo_v, wg_v, wu_v, wd_v, psib, pown, rsib, rrem,
           sw, rw, sf, rf, sa, ra, sg, rg, ss, rs, sr, rr, lsem):
    chips = n // 2
    dp, f = lax.axis_index("dp"), lax.axis_index("fsdp")
    c, k = f // 2, lax.rem(f, 2)
    par = lax.rem(dp, 2)
    partner = dp + 1 - 2 * par
    layers, seq, width = 2, x_hbm.shape[0], x_hbm.shape[1]
    blk = width // n
    tokens = n * seq
    half = tokens // 2
    ffn = wg_v.shape[2]
    part_w = ffn // 2
    heads = 4
    hd = blk // heads

    def chip(d):
        return lax.rem(c + d + chips, chips)

    def to(i):
        return (dp, chip(i // 2) * 2 + lax.rem(k + i % 2, 2))

    def source(i):
        return chip(-(i // 2)) * 2 + lax.rem(k + i % 2, 2)

    def al(v, m):
        return pl.multiple_of(v, m)

    def rc(src, dst, ssem, rsem, dev):
        return pltpu.make_async_remote_copy(src_ref=src, dst_ref=dst, send_sem=ssem, recv_sem=rsem, device_id=dev, device_id_type=MESH)

    def taken(sem, ref):
        pltpu.make_async_copy(ref, ref, sem).wait()

    def block(l, g, src, r0, rows):
        if g == QKV:
            return wqkv_v.at[l, :, pl.ds(al(src * blk + r0, 128), rows)]
        if g == WO:
            return wo_v.at[l, pl.ds(al(src * blk + r0, 16), rows), :]
        return (wg_v, wu_v)[(g - G0) // 2].at[l, pl.ds(al(src * blk + r0, 16), rows), pl.ds((g - G0) % 2 * part_w, part_w)]

    def pieces(l, g, dst, src, r0, rows):
        if g == QKV:
            cols = pl.ds(al(src * blk + r0, 128), rows)
            mine = pl.ds(al(r0, 128), rows)
            kvd = wk.shape[1] // n
            return [(wq.at[l, pl.ds(al(dst * blk, 16), blk), mine], wqkv_v.at[l, pl.ds(0, blk), cols]),
                    (wk.at[l, pl.ds(al(dst * kvd, 16), kvd), mine], wqkv_v.at[l, pl.ds(blk, kvd), cols]),
                    (wv.at[l, pl.ds(al(dst * kvd, 16), kvd), mine], wqkv_v.at[l, pl.ds(blk + kvd, kvd), cols])]
        w, at, wide = (wo, dst * blk, blk) if g == WO else ((wg, wu)[(g - G0) // 2], dst * ffn + (g - G0) % 2 * part_w, part_w)
        return [(w.at[l, pl.ds(al(r0, 16), rows), pl.ds(al(at, 128), wide)], block(l, g, src, r0, rows))]

    def bytes_of(l, g, rows):
        if g == QKV:
            return wqkv_v.at[l, :, pl.ds(0, rows)]
        if g == WO:
            return wo_v.at[l, pl.ds(0, rows), :]
        return (wg_v, wu_v)[(g - G0) // 2].at[l, pl.ds(0, rows), pl.ds((g - G0) % 2 * part_w, part_w)]

    def issue(l, g, idx):
        for i in idx:
            rows = blk if i == 1 else TAKE[l][g]
            r0 = par * (blk - rows)
            dst = to(i)
            for a, b in pieces(l, g, dst[1], f, r0, rows):
                rc(a, b, sw.at[l, g], rw.at[l, g, i], dst).start()

    def own(l, g):
        for a, b in pieces(l, g, f, f, 0, blk):
            pltpu.make_async_copy(a, b, lsem.at[l, g]).start()

    def arrived(l, g, i):
        rows = blk if i == 1 else TAKE[l][g]
        taken(rw.at[l, g, i], block(l, g, source(i), par * (blk - rows), rows))

    def forward(l, g, idx=REMOTE):
        rows = TAKE[l][g]
        for i in idx:
            if i == 1:
                continue
            arrived(l, g, i)
            if rows < blk:
                there = block(l, g, source(i), par * rows, blk - rows)
                rc(there, there, sf.at[l, g], rf.at[l, g], (partner, f)).start()

    def complete(l, g):
        taken(lsem.at[l, g], bytes_of(l, g, blk))
        arrived(l, g, 1)
        if TAKE[l][g] < blk:
            taken(rf.at[l, g], bytes_of(l, g, len(REMOTE) * (blk - TAKE[l][g])))

    def part(a, src):
        if a == AX:
            return xf.at[pl.ds(al((lax.rem(src, 2) * chips + src // 2) * seq, seq), seq), :]
        return (None, of, x1f)[a].at[:, pl.ds(al(src * blk, 128), blk)]

    def piece(a, src, i, m):
        if a == AX:
            return xf.at[pl.ds(al((lax.rem(src, 2) * chips + src // 2) * seq + i * (seq // m), seq // m), seq // m), :]
        return (None, of, x1f)[a].at[pl.ds(i * (tokens // m), tokens // m), pl.ds(al(src * blk, 128), blk)]

    def gather_start(l, a, mine=None):
        for q in range(SPLIT):
            for i in (2, 6):
                to_here = piece(a, f, q, SPLIT)
                from_here = to_here if mine is None else mine.at[pl.ds(q * (seq // SPLIT), seq // SPLIT), :]
                rc(from_here, to_here, sa.at[l, a, i], ra.at[l, a, i], to(i)).start()
        rc(part(a, f) if mine is None else mine, part(a, f), sa.at[l, a, 1], ra.at[l, a, 1], to(1)).start()

    def gather_near(l, a):
        for i, h, j in ((2, 0, 4), (6, 1, 0)):
            got = part(a, source(i))
            taken(ra.at[l, a, i], got)
            for q in range(SPLIT // 2):
                on = piece(a, source(i), h * (SPLIT // 2) + q, SPLIT)
                rc(on, on, sa.at[l, a, j], ra.at[l, a, j], to(i)).start()
            rc(got, got, sa.at[l, a, i + 1], ra.at[l, a, i + 1], to(1)).start()

    def gather_far(l, a):
        for j, h in ((4, 0), (0, 1)):
            taken(ra.at[l, a, j], piece(a, source(4), h, 2))
        got = part(a, source(4))
        rc(got, got, sa.at[l, a, 5], ra.at[l, a, 5], to(1)).start()

    def gather_end(l, a):
        for i in (1, 3, 7, 5):
            taken(ra.at[l, a, i], part(a, source(i)))
        for i in (1, 2, 3, 5, 6, 7):
            taken(sa.at[l, a, i], part(a, f))
        for j in (0, 4):
            taken(sa.at[l, a, j], piece(a, f, 0, 2))

    def norm(src, row):
        step = 32
        gain = gains[pl.ds(row, 1), :]

        @pl.loop(0, tokens // step)
        def _(i):
            at = pl.ds(al(i * step, step), step)
            v = src[at, :].astype(F32)
            inv = lax.rsqrt(jnp.mean(v * v, axis=-1, keepdims=True) + NORM_EPS)
            uf[at, :] = (v * inv * gain).astype(BF16)

    def project(l):
        step = 256

        @pl.loop(0, tokens // step)
        def _(i):
            at = pl.ds(al(i * step, step), step)
            qkvf[at, :] = lax.dot_general(uf[at, :], wqkv_v[l], (((1,), (1,)), ((), ())), preferred_element_type=F32)

    def attend(lo, hi):
        lane = lax.broadcasted_iota(jnp.int32, (seq, 128), 1)
        low = lax.rem(lane, hd) < hd // 2
        first = lane < hd
        head = lax.broadcasted_iota(jnp.int32, (seq, blk), 1) // hd
        qpos = lax.rem(lax.broadcasted_iota(jnp.int32, (heads * seq, seq), 0), seq)
        seen = qpos >= lax.broadcasted_iota(jnp.int32, (heads * seq, seq), 1)

        def rope(v):
            turned = jnp.where(low, pltpu.roll(v, 128 - hd // 2, 1), pltpu.roll(v, hd // 2, 1))
            return v * tab[0] + turned * tab[1]

        @pl.loop(lo, hi)
        def _(s):
            at = pl.ds(al(s * seq, seq), seq)
            q = jnp.concatenate([rope(qkvf[at, 0:128]), rope(qkvf[at, 128:256])], axis=1)
            kv = qkvf[at, 256:384]
            kr = rope(kv)
            k2 = jnp.where(first, kr, pltpu.roll(kr, hd, 1)).astype(BF16)
            v2 = jnp.where(first, pltpu.roll(kv, hd, 1), kv).astype(BF16)
            k4 = jnp.concatenate([k2, k2], axis=1)
            v4 = jnp.concatenate([v2, v2], axis=1)
            q4 = jnp.concatenate([jnp.where(head == h, q, 0.0) for h in range(heads)], axis=0).astype(BF16)
            score = lax.dot_general(q4, k4, (((1,), (1,)), ((), ())), preferred_element_type=F32) * hd ** -0.5
            score = jnp.where(seen, score, -jnp.inf)
            e = jnp.exp(score - jnp.max(score, axis=-1, keepdims=True))
            prob = (e / jnp.sum(e, axis=-1, keepdims=True)).astype(BF16)
            o4 = jnp.dot(prob, v4, preferred_element_type=F32)
            o = o4[0:seq]
            for h in range(1, heads):
                o = jnp.where(head == h, o4[h * seq:(h + 1) * seq], o)
            of[at, pl.ds(al(f * blk, 128), blk)] = o.astype(BF16)

    def output_projection(l):
        step = 256

        @pl.loop(0, tokens // step)
        def _(i):
            at = pl.ds(al(i * step, step), step)
            cols = pl.ds(al(f * blk, 128), blk)
            acc = jnp.dot(of[at, :], wo_v[l], preferred_element_type=F32)
            x1f[at, cols] = (xf[at, cols].astype(F32) + acc).astype(BF16)

    def gate_up(l, h):
        step = 256

        @pl.loop(h * part_w // step, (h + 1) * part_w // step)
        def _(i):
            at = pl.ds(al(i * step, step), step)
            a = jnp.dot(uf[...], wg_v[l, :, at], preferred_element_type=F32).astype(BF16).astype(F32)
            b = jnp.dot(uf[...], wu_v[l, :, at], preferred_element_type=F32).astype(BF16).astype(F32)
            zf[:, at] = (a * jax.nn.sigmoid(a) * b).astype(BF16)

    dtile = width // 4
    ptile = width // TILES
    per = TILES // 4

    def pcols(p):
        return pl.ds(p * ptile, ptile)

    def side(p):
        return 2 * p % 4 - 1

    def hop(s):
        return 2 if s == 1 else 6

    def rows_of(d):
        return pl.ds(al(chip(d) * seq, seq), seq)

    def down_start(l):
        for t in range(4):
            cols = pl.ds(t * dtile, dtile)
            psib[:, cols] = jnp.dot(zf[pl.ds(al((1 - k) * half, half), half), :], wd_v[l, :, cols], preferred_element_type=F32)
            rc(psib.at[:, cols], rsib.at[:, cols], ss.at[l, t], rs.at[l, t], to(1)).start()
        for t in range(4):
            cols = pl.ds(t * dtile, dtile)
            acc = jnp.dot(zf[pl.ds(al(k * half, half), half), :], wd_v[l, :, cols], preferred_element_type=F32)
            taken(rs.at[l, t], rsib.at[:, cols])
            pown[:, cols] = acc + rsib[:, cols]
            for p in range(t * per, (t + 1) * per):
                s = side(p)
                rc(pown.at[rows_of(2), pcols(p)], rrem.at[0, :, pcols(p)], sr.at[l, p, 0], rr.at[l, p, 0], to(hop(s))).start()
                rc(pown.at[rows_of(-s), pcols(p)], rrem.at[1, :, pcols(p)], sr.at[l, p, 1], rr.at[l, p, 1], to(hop(-s))).start()

    def down_pass(l):
        for p in range(TILES):
            s = side(p)
            taken(rr.at[l, p, 0], rrem.at[0, :, pcols(p)])
            pown[rows_of(s), pcols(p)] += rrem[0, :, pcols(p)]
            rc(pown.at[rows_of(s), pcols(p)], rrem.at[2, :, pcols(p)], sr.at[l, p, 2], rr.at[l, p, 2], to(hop(s))).start()

    def down_end(l, out):
        at = pl.ds(al((k * chips + c) * seq, seq), seq)
        for p in range(TILES):
            for j in (1, 2):
                taken(rr.at[l, p, j], rrem.at[j, :, pcols(p)])
            acc = pown[rows_of(0), pcols(p)] + rrem[1, :, pcols(p)] + rrem[2, :, pcols(p)]
            out(pcols(p), (x1f[at, pcols(p)].astype(F32) + acc).astype(BF16))

    def down_sent(l):
        for t in range(4):
            taken(ss.at[l, t], psib.at[:, pl.ds(t * dtile, dtile)])
        for p in range(TILES):
            for j in range(3):
                taken(sr.at[l, p, j], rrem.at[j, :, pcols(p)])

    gains[...] = jnp.zeros_like(gains)
    mycols = pl.ds(al(f * blk, 128), blk)
    gains[0:2, mycols] = an_ref[...].astype(F32)
    gains[2:4, mycols] = mn_ref[...].astype(F32)
    gblock = gains.at[:, mycols]
    local_x = pltpu.make_async_copy(x_hbm, part(AX, f), lsem.at[0, 6])
    local_x.start()
    local_tab = pltpu.make_async_copy(tab_hbm, tab, lsem.at[1, 6])
    local_tab.start()
    own(0, QKV)

    barrier = pltpu.get_barrier_semaphore()
    for i in range(1, n):
        pl.semaphore_signal(barrier, inc=1, device_id=to(i), device_id_type=MESH)
    pl.semaphore_signal(barrier, inc=1, device_id=(partner, f), device_id_type=MESH)
    pl.semaphore_wait(barrier, n)

    issue(0, WO, ALL)
    issue(0, G0, ALL)
    gather_start(0, AX, x_hbm)
    for i in range(1, n):
        rc(gblock, gblock, sg.at[i], rg.at[i], to(i)).start()
    issue(0, QKV, ALL)
    for g in (WO, G0, G1, U0, U1):
        own(0, g)
    own_d = [pltpu.make_async_copy(wd.at[l], wd_v.at[l], lsem.at[l, 7]) for l in range(layers)]
    own_d[0].start()
    forward(0, WO)
    forward(0, G0)

    for l in range(layers):
        last = l + 1 == layers
        gather_near(l, AX)
        if l == 0:
            issue(l, G1, ALL)
            forward(l, QKV)
            gather_far(l, AX)
            local_x.wait()
            local_tab.wait()
            for i in range(1, n):
                taken(rg.at[i], gains.at[:, pl.ds(al(source(i) * blk, 128), blk)])
        else:
            issue(l, G0, CROSS)
            issue(l, G1, FAR)
            issue(l, G1, NEAR)
            gather_far(l, AX)
            forward(l, G0, NEAR)
        gather_end(l, AX)
        norm(xf, l)
        if l == 0:
            issue(l, U0, ALL)
            forward(l, G1)
        complete(l, QKV)
        project(l)
        attend(0, n // 2)
        if l > 0:
            forward(l, G1, FAR)
        attend(n // 2, n)
        gather_start(l, AO)
        if l == 0:
            issue(l, U1, SAME)
            forward(l, U0)
            gather_near(l, AO)
            issue(l, U1, CROSS)
            issue(l, U1, FAR)
            forward(l, U1, SAME)
            gather_far(l, AO)
            forward(l, U1, CROSS)
        else:
            issue(l, U0, SAME)
            forward(l, G1, NEAR)
            gather_near(l, AO)
            issue(l, U0, CROSS)
            issue(l, U0, FAR)
            issue(l, U1, FAR)
            forward(l, U0, SAME)
            gather_far(l, AO)
            forward(l, U0, CROSS)
        gather_end(l, AO)
        complete(l, WO)
        output_projection(l)
        gather_start(l, AM)
        if l == 0:
            forward(l, U1, FAR)
            gather_near(l, AM)
            for part_of in (NEAR, FAR):
                issue(l + 1, QKV, part_of)
                issue(l + 1, WO, part_of)
            for g in range(GROUPS):
                own(l + 1, g)
            own_d[l + 1].start()
            gather_far(l, AM)
        else:
            issue(l, U1, SAME)
            forward(l, U0, FAR)
            forward(l, U1, FAR)
            gather_near(l, AM)
            issue(l, U1, CROSS)
            forward(l, U1, SAME)
            gather_far(l, AM)
            forward(l, U1, CROSS)
        gather_end(l, AM)
        norm(x1f, layers + l)
        complete(l, G0)
        complete(l, U0)
        gate_up(l, 0)
        complete(l, G1)
        complete(l, U1)
        gate_up(l, 1)
        own_d[l].wait()
        down_start(l)
        if not last:
            def store(cols, v):
                xf[pl.ds(al((k * chips + c) * seq, seq), seq), cols] = v

            forward(l + 1, QKV)
            forward(l + 1, WO)
            down_pass(l)
            issue(l + 1, G0, FAR)
            down_end(l, store)
            down_sent(l)
            gather_start(l + 1, AX)
            issue(l + 1, G0, SAME)
            forward(l + 1, G0, FAR)
        else:
            def store(cols, v):
                y_ref[:, cols] = v

            down_pass(l)
            down_end(l, store)
            down_sent(l)

    for i in range(1, n):
        taken(sg.at[i], gblock)
    for l in range(layers):
        for g in range(GROUPS):
            taken(sw.at[l, g], bytes_of(l, g, len(REMOTE) * TAKE[l][g] + blk))
            if TAKE[l][g] < blk:
                taken(sf.at[l, g], bytes_of(l, g, len(REMOTE) * (blk - TAKE[l][g])))


def rope_tables(seq, hd):
    inv_freq = np.power(np.float32(ROPE_THETA), -(np.arange(hd // 2, dtype=np.float32) * np.float32(2.0) / np.float32(hd)))
    angles = np.arange(seq, dtype=np.float32)[:, None] * inv_freq[None, :].astype(np.float32)
    cos, sin = np.cos(angles), np.sin(angles)
    cos = np.concatenate([cos, cos] * (128 // hd), axis=1)
    sin = np.concatenate([-sin, sin] * (128 // hd), axis=1)
    return np.stack([cos, sin]).astype(np.float32)


def solution(mesh):
    n = mesh.shape["fsdp"]
    batch_spec = P(("dp", "fsdp"), None, None)
    gain_spec = P(None, "fsdp")
    proj_spec = P(None, "fsdp", None, None)
    mat_spec = P(None, "fsdp", None)

    def local_forward(hidden, attn_norm, w_q, w_k, w_v, w_o, mlp_norm, w_gate, w_up, w_down):
        seq, width = hidden.shape[1], hidden.shape[2]
        layers, blk, hd = w_q.shape[0], w_q.shape[1], w_q.shape[3]
        tokens, ffn = n * seq, w_gate.shape[2] // n
        half = tokens // 2
        qkv = (w_q.shape[2] + 2 * w_k.shape[2]) * hd // n

        def turn(w):
            return jnp.transpose(w, (0, 2, 3, 1)).reshape(layers, w.shape[2] * hd, blk)

        tables = jnp.asarray(rope_tables(seq, hd))
        anyspace = pl.BlockSpec(memory_space=pl.ANY)
        vmem = pl.BlockSpec(memory_space=pltpu.VMEM)
        dma = pltpu.SemaphoreType.DMA
        out = pl.pallas_call(
            functools.partial(kernel, n),
            out_shape=jax.ShapeDtypeStruct((seq, width), BF16),
            in_specs=[anyspace, vmem, vmem] + [anyspace] * 8,
            out_specs=vmem,
            scratch_shapes=[
                pltpu.VMEM((tokens, width), BF16),
                pltpu.VMEM((tokens, width), BF16),
                pltpu.VMEM((tokens, width), BF16),
                pltpu.VMEM((tokens, width), BF16),
                pltpu.VMEM((tokens, qkv), F32),
                pltpu.VMEM((tokens, ffn), BF16),
                pltpu.VMEM((8, width), F32),
                pltpu.VMEM((2, seq, 128), F32),
                pltpu.VMEM((layers, qkv, width), BF16),
                pltpu.VMEM((layers, width, blk), BF16),
                pltpu.VMEM((layers, width, ffn), BF16),
                pltpu.VMEM((layers, width, ffn), BF16),
                pltpu.VMEM((layers, ffn, width), BF16),
                pltpu.VMEM((half, width), F32),
                pltpu.VMEM((half, width), F32),
                pltpu.VMEM((half, width), F32),
                pltpu.VMEM((3, seq, width), F32),
                dma((layers, GROUPS)), dma((layers, GROUPS, n)),
                dma((layers, GROUPS)), dma((layers, GROUPS)),
                dma((layers, 3, n)), dma((layers, 3, n)),
                dma((n,)), dma((n,)),
                dma((layers, 4)), dma((layers, 4)),
                dma((layers, TILES, 3)), dma((layers, TILES, 3)),
                dma((layers, 8)),
            ],
            compiler_params=pltpu.CompilerParams(collective_id=0, has_side_effects=True, vmem_limit_bytes=63 * 2**20),
        )(hidden[0], attn_norm, mlp_norm, tables, turn(w_q), turn(w_k), turn(w_v), w_o, w_gate, w_up, w_down)
        return out[None]

    return jax.shard_map(local_forward, mesh=mesh, in_specs=(batch_spec, gain_spec, proj_spec, proj_spec, proj_spec, mat_spec, gain_spec, mat_spec, mat_spec, mat_spec), out_specs=batch_spec, check_vma=False)
```

```python
import functools

import jax
import jax.numpy as jnp
import numpy as np
from jax import lax
from jax.experimental import pallas as pl
from jax.experimental.pallas import tpu as pltpu
from jax.sharding import PartitionSpec as P

ROPE_THETA = 500000.0
NORM_EPS = 1e-5
MESH = pl.DeviceIdType.MESH
F32 = jnp.float32
BF16 = jnp.bfloat16

QKV, WO, G0, G1, U0, U1 = range(6)
AX, AO, AM = range(3)
REMOTE = (2, 3, 6, 7, 4, 5)
SAME, CROSS, FAR, OTHER = (2, 6), (3, 7), (4, 5), (1,)
GROUPS = 6
SPLIT = 4
TILES = 8
SEQS = 2
NROWS = 32
STEPS = 4
AHEAD = 2
WHOLE = ()


def kernel(n, x_hbm, an_ref, mn_ref, tab_hbm, wq, wk, wv, wo, wg, wu, wd, y_hbm,
           xf, of, x1f, uf, qkvf, zf, gains, tab, wqkv_v, wo_v, wg_v, wu_v, wd_v, yv, psib, pown, rsib, rrem,
           sw, rw, sf, rf, sa, ra, sg, rg, ss, rs, sr, rr, lsem):
    chips = n // 2
    dp, f = lax.axis_index("dp"), lax.axis_index("fsdp")
    c, k = f // 2, lax.rem(f, 2)
    par = lax.rem(dp, 2)
    partner = dp + 1 - 2 * par
    layers, seq, width = 2, x_hbm.shape[0], x_hbm.shape[1]
    blk = width // n
    tokens = n * seq
    half = tokens // 2
    ffn = wg_v.shape[2]
    part_w = ffn // 2
    heads = 4
    hd = blk // heads

    def chip(d):
        return lax.rem(c + d + chips, chips)

    def to(i):
        return (dp, chip(i // 2) * 2 + lax.rem(k + i % 2, 2))

    def source(i):
        return chip(-(i // 2)) * 2 + lax.rem(k + i % 2, 2)

    def al(v, m):
        return pl.multiple_of(v, m)

    def rc(src, dst, ssem, rsem, dev):
        return pltpu.make_async_remote_copy(src_ref=src, dst_ref=dst, send_sem=ssem, recv_sem=rsem, device_id=dev, device_id_type=MESH)

    def taken(sem, ref):
        pltpu.make_async_copy(ref, ref, sem).wait()

    def block(l, g, src, r0, rows):
        if g == QKV:
            return wqkv_v.at[l, :, pl.ds(al(src * blk + r0, 128), rows)]
        if g == WO:
            return wo_v.at[l, pl.ds(al(src * blk + r0, 16), rows), :]
        return (wg_v, wu_v)[(g - G0) // 2].at[l, pl.ds(al(src * blk + r0, 16), rows), pl.ds((g - G0) % 2 * part_w, part_w)]

    def pieces(l, g, dst, src, r0, rows):
        if g == QKV:
            cols = pl.ds(al(src * blk + r0, 128), rows)
            mine = pl.ds(al(r0, 128), rows)
            kvd = wk.shape[1] // n
            return [(wq.at[l, pl.ds(al(dst * blk, 16), blk), mine], wqkv_v.at[l, pl.ds(0, blk), cols]),
                    (wk.at[l, pl.ds(al(dst * kvd, 16), kvd), mine], wqkv_v.at[l, pl.ds(blk, kvd), cols]),
                    (wv.at[l, pl.ds(al(dst * kvd, 16), kvd), mine], wqkv_v.at[l, pl.ds(blk + kvd, kvd), cols])]
        w, at, wide = (wo, dst * blk, blk) if g == WO else ((wg, wu)[(g - G0) // 2], dst * ffn + (g - G0) % 2 * part_w, part_w)
        return [(w.at[l, pl.ds(al(r0, 16), rows), pl.ds(al(at, 128), wide)], block(l, g, src, r0, rows))]

    def bytes_of(l, g, rows):
        if g == QKV:
            return wqkv_v.at[l, :, pl.ds(0, rows)]
        if g == WO:
            return wo_v.at[l, pl.ds(0, rows), :]
        return (wg_v, wu_v)[(g - G0) // 2].at[l, pl.ds(0, rows), pl.ds((g - G0) % 2 * part_w, part_w)]

    def take(l, g, i):
        return blk if i == 1 or (l, g, i) in WHOLE else blk // 2

    def brought(l, g):
        return sum(blk - take(l, g, i) for i in REMOTE)

    def issue(l, g, idx):
        for i in idx:
            rows = take(l, g, i)
            r0 = par * (blk - rows)
            dst = to(i)
            for a, b in pieces(l, g, dst[1], f, r0, rows):
                rc(a, b, sw.at[l, g], rw.at[l, g, slot(i)], dst).start()

    def own(l, g):
        for a, b in pieces(l, g, f, f, 0, blk):
            pltpu.make_async_copy(a, b, lsem.at[l, g]).start()

    def slot(i):
        return (0, 0, 0, 1, 2, 2, 0, 1)[i] if i > 1 else 3

    def arrived(l, g, idx):
        taken(rw.at[l, g, slot(idx[0])], bytes_of(l, g, sum(take(l, g, i) for i in idx)))

    def forward(l, g, idx=REMOTE):
        arrived(l, g, idx)
        for i in idx:
            rows = take(l, g, i)
            if rows < blk:
                there = block(l, g, source(i), par * rows, blk - rows)
                rc(there, there, sf.at[l, g], rf.at[l, g], (partner, f)).start()

    def complete(l, g):
        taken(lsem.at[l, g], bytes_of(l, g, blk))
        arrived(l, g, OTHER)
        taken(rf.at[l, g], bytes_of(l, g, brought(l, g)))

    def part(a, src):
        if a == AX:
            return xf.at[pl.ds(al((lax.rem(src, 2) * chips + src // 2) * seq, seq), seq), :]
        return (None, of, x1f)[a].at[:, pl.ds(al(src * blk, 128), blk)]

    def piece(a, src, i, m):
        if a == AX:
            return xf.at[pl.ds(al((lax.rem(src, 2) * chips + src // 2) * seq + i * (seq // m), seq // m), seq // m), :]
        return (None, of, x1f)[a].at[pl.ds(i * (tokens // m), tokens // m), pl.ds(al(src * blk, 128), blk)]

    def gather_start(l, a, mine=None):
        for q in range(SPLIT):
            for i in (2, 6):
                to_here = piece(a, f, q, SPLIT)
                from_here = to_here if mine is None else mine.at[pl.ds(q * (seq // SPLIT), seq // SPLIT), :]
                rc(from_here, to_here, sa.at[a], ra.at[a, i], to(i)).start()
        rc(part(a, f) if mine is None else mine, part(a, f), sa.at[a], ra.at[a, 1], to(1)).start()

    def gather_near(l, a):
        for i, h, j in ((2, 0, 4), (6, 1, 0)):
            got = part(a, source(i))
            taken(ra.at[a, i], got)
            for q in range(SPLIT // 2):
                on = piece(a, source(i), h * (SPLIT // 2) + q, SPLIT)
                rc(on, on, sa.at[a], ra.at[a, j], to(i)).start()
            rc(got, got, sa.at[a], ra.at[a, i + 1], to(1)).start()

    def gather_far(l, a):
        for j, h in ((4, 0), (0, 1)):
            taken(ra.at[a, j], piece(a, source(4), h, 2))
        got = part(a, source(4))
        rc(got, got, sa.at[a], ra.at[a, 5], to(1)).start()

    def gather_end(l, a):
        for i in (1, 3, 7, 5):
            taken(ra.at[a, i], part(a, source(i)))
        taken(sa.at[a], xf.at[pl.ds(0, (n - 1) * seq), :] if a == AX else of.at[:, pl.ds(0, (n - 1) * blk)])

    def norm(src, row):
        step = NROWS
        gain = gains[pl.ds(row, 1), :]

        @pl.loop(0, tokens // step)
        def _(i):
            at = pl.ds(al(i * step, step), step)
            v = src[at, :].astype(F32)
            inv = lax.rsqrt(jnp.mean(v * v, axis=-1, keepdims=True) + NORM_EPS)
            uf[at, :] = (v * inv * gain).astype(BF16)

    def project(l):
        step = 256

        @pl.loop(0, tokens // step)
        def _(i):
            at = pl.ds(al(i * step, step), step)
            qkvf[at, :] = lax.dot_general(uf[at, :], wqkv_v[l], (((1,), (1,)), ((), ())), preferred_element_type=F32)

    def attend(lo, hi):
        lane = lax.broadcasted_iota(jnp.int32, (seq, 128), 1)
        low = lax.rem(lane, hd) < hd // 2
        first = lane < hd
        head = lax.broadcasted_iota(jnp.int32, (seq, blk), 1) // hd
        qpos = lax.rem(lax.broadcasted_iota(jnp.int32, (heads * seq, seq), 0), seq)
        seen = qpos >= lax.broadcasted_iota(jnp.int32, (heads * seq, seq), 1)

        def rope(v):
            turned = jnp.where(low, pltpu.roll(v, 128 - hd // 2, 1), pltpu.roll(v, hd // 2, 1))
            return v * tab[0] + turned * tab[1]

        def one(s):
            at = pl.ds(al(s * seq, seq), seq)
            q = jnp.concatenate([rope(qkvf[at, 0:128]), rope(qkvf[at, 128:256])], axis=1)
            kv = qkvf[at, 256:384]
            kr = rope(kv)
            k2 = jnp.where(first, kr, pltpu.roll(kr, hd, 1)).astype(BF16)
            v2 = jnp.where(first, pltpu.roll(kv, hd, 1), kv).astype(BF16)
            k4 = jnp.concatenate([k2, k2], axis=1)
            v4 = jnp.concatenate([v2, v2], axis=1)
            q4 = jnp.concatenate([jnp.where(head == h, q, 0.0) for h in range(heads)], axis=0).astype(BF16)
            score = lax.dot_general(q4, k4, (((1,), (1,)), ((), ())), preferred_element_type=F32) * hd ** -0.5
            score = jnp.where(seen, score, -jnp.inf)
            e = jnp.exp(score - jnp.max(score, axis=-1, keepdims=True))
            prob = (e / jnp.sum(e, axis=-1, keepdims=True)).astype(BF16)
            o4 = jnp.dot(prob, v4, preferred_element_type=F32)
            o = o4[0:seq]
            for h in range(1, heads):
                o = jnp.where(head == h, o4[h * seq:(h + 1) * seq], o)
            return at, o.astype(BF16)

        @pl.loop(lo // SEQS, hi // SEQS)
        def _(i):
            done = [one(i * SEQS + j) for j in range(SEQS)]
            for at, o in done:
                of[at, pl.ds(al(f * blk, 128), blk)] = o

    def output_projection(l):
        step = 256

        @pl.loop(0, tokens // step)
        def _(i):
            at = pl.ds(al(i * step, step), step)
            cols = pl.ds(al(f * blk, 128), blk)
            acc = jnp.dot(of[at, :], wo_v[l], preferred_element_type=F32)
            x1f[at, cols] = (xf[at, cols].astype(F32) + acc).astype(BF16)

    def gate_up(l, h):
        step = 256

        @pl.loop(h * part_w // step, (h + 1) * part_w // step)
        def _(i):
            at = pl.ds(al(i * step, step), step)
            a = jnp.dot(uf[...], wg_v[l, :, at], preferred_element_type=F32).astype(BF16).astype(F32)
            b = jnp.dot(uf[...], wu_v[l, :, at], preferred_element_type=F32).astype(BF16).astype(F32)
            zf[:, at] = (a * jax.nn.sigmoid(a) * b).astype(BF16)

    ptile = width // TILES
    dtile = width // STEPS
    per = TILES // STEPS

    def pcols(p):
        return pl.ds(p * ptile, ptile)

    def side(p):
        return 2 * p % 4 - 1

    def hop(s):
        return 2 if s == 1 else 6

    def rows_of(d):
        return pl.ds(al(chip(d) * seq, seq), seq)

    def down_start(l):
        def theirs(t):
            cols = pl.ds(t * dtile, dtile)
            psib[:, cols] = jnp.dot(zf[pl.ds(al((1 - k) * half, half), half), :], wd_v[l, :, cols], preferred_element_type=F32)
            rc(psib.at[:, cols], rsib.at[:, cols], ss, rs.at[t], to(1)).start()

        for t in range(AHEAD):
            theirs(t)
        for t in range(STEPS):
            cols = pl.ds(t * dtile, dtile)
            acc = jnp.dot(zf[pl.ds(al(k * half, half), half), :], wd_v[l, :, cols], preferred_element_type=F32)
            taken(rs.at[t], rsib.at[:, cols])
            pown[:, cols] = acc + rsib[:, cols]
            for p in range(t * per, (t + 1) * per):
                s = side(p)
                rc(pown.at[rows_of(2), pcols(p)], rrem.at[0, :, pcols(p)], sr, rr.at[p, 0], to(hop(s))).start()
                rc(pown.at[rows_of(-s), pcols(p)], rrem.at[1, :, pcols(p)], sr, rr.at[p, 1], to(hop(-s))).start()
            if t + AHEAD < STEPS:
                theirs(t + AHEAD)

    def down_pass(l):
        for p in range(TILES):
            s = side(p)
            taken(rr.at[p, 0], rrem.at[0, :, pcols(p)])
            pown[rows_of(s), pcols(p)] += rrem[0, :, pcols(p)]
            rc(pown.at[rows_of(s), pcols(p)], rrem.at[2, :, pcols(p)], sr, rr.at[p, 2], to(hop(s))).start()

    def down_end(l, out):
        at = pl.ds(al((k * chips + c) * seq, seq), seq)
        for p in range(TILES):
            for j in (1, 2):
                taken(rr.at[p, j], rrem.at[j, :, pcols(p)])
            acc = pown[rows_of(0), pcols(p)] + rrem[1, :, pcols(p)] + rrem[2, :, pcols(p)]
            out(pcols(p), (x1f[at, pcols(p)].astype(F32) + acc).astype(BF16))

    def down_sent(l):
        taken(ss, psib)
        taken(sr, rrem)

    gains[...] = jnp.zeros_like(gains)
    mycols = pl.ds(al(f * blk, 128), blk)
    gains[0:2, mycols] = an_ref[...].astype(F32)
    gains[2:4, mycols] = mn_ref[...].astype(F32)
    gblock = gains.at[:, mycols]
    local_x = pltpu.make_async_copy(x_hbm, part(AX, f), lsem.at[0, 6])
    local_x.start()
    local_tab = pltpu.make_async_copy(tab_hbm, tab, lsem.at[1, 6])
    local_tab.start()
    own(0, QKV)

    barrier = pltpu.get_barrier_semaphore()
    for i in range(1, n):
        pl.semaphore_signal(barrier, inc=1, device_id=to(i), device_id_type=MESH)
    pl.semaphore_signal(barrier, inc=1, device_id=(partner, f), device_id_type=MESH)
    pl.semaphore_wait(barrier, n)

    def load_down(l):
        pltpu.make_async_copy(wd.at[l], wd_v.at[l], lsem.at[l, 7]).start()

    def send_gains():
        for i in range(1, n):
            rc(gblock, gblock, sg, rg, to(i)).start()

    def local_ready():
        local_x.wait()
        local_tab.wait()
        taken(rg, gains.at[:, pl.ds(0, (n - 1) * blk)])

    def own_all(l, groups):
        for g in groups:
            own(l, g)
        load_down(l)

    def down_ready(l):
        taken(lsem.at[l, 7], wd_v.at[l])

    def keep(cols, v):
        xf[pl.ds(al((k * chips + c) * seq, seq), seq), cols] = v

    def emit(cols, v):
        yv[:, cols] = v
        pltpu.make_async_copy(yv.at[:, cols], y_hbm.at[:, cols], lsem.at[1, 7]).start()

    issue(0, WO, SAME)
    issue(0, WO, CROSS)
    issue(0, WO, FAR)
    issue(0, WO, OTHER)
    issue(0, G0, SAME)
    issue(0, G0, CROSS)
    issue(0, G0, FAR)
    issue(0, G0, OTHER)
    gather_start(0, AX, x_hbm)
    send_gains()
    issue(0, QKV, SAME)
    issue(0, QKV, CROSS)
    issue(0, QKV, FAR)
    issue(0, QKV, OTHER)
    own_all(0, (WO, G0, G1, U0, U1))
    forward(0, WO, SAME)
    forward(0, WO, CROSS)
    forward(0, WO, FAR)
    forward(0, G0, SAME)
    forward(0, G0, CROSS)
    forward(0, G0, FAR)
    gather_near(0, AX)
    issue(0, G1, SAME)
    issue(0, G1, CROSS)
    issue(0, G1, FAR)
    issue(0, G1, OTHER)
    forward(0, QKV, SAME)
    forward(0, QKV, CROSS)
    forward(0, QKV, FAR)
    gather_far(0, AX)
    local_ready()
    gather_end(0, AX)
    norm(xf, 0)
    issue(0, U0, SAME)
    issue(0, U0, CROSS)
    issue(0, U0, FAR)
    issue(0, U0, OTHER)
    forward(0, G1, SAME)
    forward(0, G1, CROSS)
    forward(0, G1, FAR)
    complete(0, QKV)
    project(0)
    attend(0, n // 2)
    attend(n // 2, n)
    gather_start(0, AO)
    issue(0, U1, SAME)
    forward(0, U0, SAME)
    forward(0, U0, CROSS)
    forward(0, U0, FAR)
    gather_near(0, AO)
    issue(0, U1, CROSS)
    issue(0, U1, FAR)
    issue(0, U1, OTHER)
    forward(0, U1, SAME)
    gather_far(0, AO)
    gather_end(0, AO)
    complete(0, WO)
    output_projection(0)
    gather_start(0, AM)
    forward(0, U1, CROSS)
    forward(0, U1, FAR)
    gather_near(0, AM)
    issue(1, QKV, SAME)
    issue(1, QKV, CROSS)
    issue(1, WO, SAME)
    issue(1, WO, CROSS)
    issue(1, QKV, FAR)
    issue(1, QKV, OTHER)
    issue(1, WO, FAR)
    issue(1, WO, OTHER)
    own_all(1, range(GROUPS))
    gather_far(0, AM)
    gather_end(0, AM)
    norm(x1f, layers + 0)
    complete(0, G0)
    complete(0, U0)
    gate_up(0, 0)
    complete(0, G1)
    complete(0, U1)
    gate_up(0, 1)
    down_ready(0)
    down_start(0)
    forward(1, QKV, SAME)
    forward(1, QKV, CROSS)
    forward(1, QKV, FAR)
    forward(1, WO, SAME)
    forward(1, WO, CROSS)
    forward(1, WO, FAR)
    down_pass(0)
    issue(1, G0, SAME)
    issue(1, G0, CROSS)
    down_end(0, keep)
    down_sent(0)
    gather_start(1, AX)
    issue(1, U0, SAME)
    forward(1, G0, SAME)
    forward(1, G0, CROSS)
    gather_near(1, AX)
    issue(1, U0, CROSS)
    issue(1, G0, FAR)
    issue(1, G0, OTHER)
    issue(1, G1, SAME)
    issue(1, G1, CROSS)
    gather_far(1, AX)
    issue(1, G1, FAR)
    issue(1, G1, OTHER)
    forward(1, U0, SAME)
    gather_end(1, AX)
    norm(xf, 1)
    complete(1, QKV)
    project(1)
    forward(1, U0, CROSS)
    attend(0, n // 2)
    forward(1, G0, FAR)
    attend(n // 2, n)
    gather_start(1, AO)
    issue(1, U1, SAME)
    forward(1, G1, SAME)
    forward(1, G1, CROSS)
    gather_near(1, AO)
    issue(1, U1, CROSS)
    forward(1, G1, FAR)
    forward(1, U1, SAME)
    gather_far(1, AO)
    issue(1, U0, FAR)
    issue(1, U0, OTHER)
    issue(1, U1, FAR)
    issue(1, U1, OTHER)
    gather_end(1, AO)
    complete(1, WO)
    output_projection(1)
    gather_start(1, AM)
    forward(1, U1, CROSS)
    forward(1, U0, FAR)
    forward(1, U1, FAR)
    gather_near(1, AM)
    gather_far(1, AM)
    gather_end(1, AM)
    norm(x1f, layers + 1)
    complete(1, G0)
    complete(1, U0)
    gate_up(1, 0)
    complete(1, G1)
    complete(1, U1)
    gate_up(1, 1)
    down_ready(1)
    down_start(1)
    down_pass(1)
    down_end(1, emit)
    down_sent(1)
    taken(lsem.at[1, 7], yv)
    taken(sg, gains.at[:, pl.ds(0, (n - 1) * blk)])
    for l in range(layers):
        for g in range(GROUPS):
            taken(sw.at[l, g], bytes_of(l, g, n * blk - blk - brought(l, g)))
            taken(sf.at[l, g], bytes_of(l, g, brought(l, g)))


def rope_tables(seq, hd):
    inv_freq = np.power(np.float32(ROPE_THETA), -(np.arange(hd // 2, dtype=np.float32) * np.float32(2.0) / np.float32(hd)))
    angles = np.arange(seq, dtype=np.float32)[:, None] * inv_freq[None, :].astype(np.float32)
    cos, sin = np.cos(angles), np.sin(angles)
    cos = np.concatenate([cos, cos] * (128 // hd), axis=1)
    sin = np.concatenate([-sin, sin] * (128 // hd), axis=1)
    return np.stack([cos, sin]).astype(np.float32)


def solution(mesh):
    n = mesh.shape["fsdp"]
    batch_spec = P(("dp", "fsdp"), None, None)
    gain_spec = P(None, "fsdp")
    proj_spec = P(None, "fsdp", None, None)
    mat_spec = P(None, "fsdp", None)

    def local_forward(hidden, attn_norm, w_q, w_k, w_v, w_o, mlp_norm, w_gate, w_up, w_down):
        seq, width = hidden.shape[1], hidden.shape[2]
        layers, blk, hd = w_q.shape[0], w_q.shape[1], w_q.shape[3]
        tokens, ffn = n * seq, w_gate.shape[2] // n
        half = tokens // 2
        qkv = (w_q.shape[2] + 2 * w_k.shape[2]) * hd // n

        def turn(w):
            return jnp.transpose(w, (0, 2, 3, 1)).reshape(layers, w.shape[2] * hd, blk)

        tables = jnp.asarray(rope_tables(seq, hd))
        anyspace = pl.BlockSpec(memory_space=pl.ANY)
        vmem = pl.BlockSpec(memory_space=pltpu.VMEM)
        dma = pltpu.SemaphoreType.DMA
        out = pl.pallas_call(
            functools.partial(kernel, n),
            out_shape=jax.ShapeDtypeStruct((seq, width), BF16),
            in_specs=[anyspace, vmem, vmem] + [anyspace] * 8,
                out_specs=anyspace,
            scratch_shapes=[
                pltpu.VMEM((tokens, width), BF16),
                pltpu.VMEM((tokens, width), BF16),
                pltpu.VMEM((tokens, width), BF16),
                pltpu.VMEM((tokens, width), BF16),
                pltpu.VMEM((tokens, qkv), F32),
                pltpu.VMEM((tokens, ffn), BF16),
                pltpu.VMEM((8, width), F32),
                pltpu.VMEM((2, seq, 128), F32),
                pltpu.VMEM((layers, qkv, width), BF16),
                pltpu.VMEM((layers, width, blk), BF16),
                pltpu.VMEM((layers, width, ffn), BF16),
                pltpu.VMEM((layers, width, ffn), BF16),
                pltpu.VMEM((layers, ffn, width), BF16),
                pltpu.VMEM((seq, width), BF16),
                pltpu.VMEM((half, width), F32),
                pltpu.VMEM((half, width), F32),
                pltpu.VMEM((half, width), F32),
                pltpu.VMEM((3, seq, width), F32),
                dma((layers, GROUPS)), dma((layers, GROUPS, 4)),
                dma((layers, GROUPS)), dma((layers, GROUPS)),
                dma((3,)), dma((3, n)),
                dma, dma,
                dma, dma((STEPS,)),
                dma, dma((TILES, 3)),
                dma((layers, 8)),
            ],
            compiler_params=pltpu.CompilerParams(collective_id=0, has_side_effects=True, vmem_limit_bytes=63 * 2**20),
        )(hidden[0], attn_norm, mlp_norm, tables, turn(w_q), turn(w_k), turn(w_v), w_o, w_gate, w_up, w_down)
        return out[None]

    return jax.shard_map(local_forward, mesh=mesh, in_specs=(batch_spec, gain_spec, proj_spec, proj_spec, proj_spec, mat_spec, gain_spec, mat_spec, mat_spec, mat_spec), out_specs=batch_spec, check_vma=False)
```
